32 devices in a mesh: node: 8 (over z, x), freq: 4 (over y, core).
Axes of the slice: x: 2, y: 2, z: 4, core: 2. Of those that a mesh axis runs over, the one named last changes fastest.
Arguments:
- action_old: float32 [36, 36, 4096], P('freq', None, 'node'), may hold values from 0.05 to 2
- source: float32 [36, 36, 4096], P('freq', None, 'node'), may hold values from -4 to 4
- time_weight: float32 [4096], P('node'), may hold values from 0.5 to 4
- group_speed: float32 [36], P('freq'), may hold values from 0.3 to 3
- normals: float32 [2, 8, 4096], P(None, None, 'node'), may hold values from -3 to 3
- refract: float32 [4096], P('node'), may hold values from -4 to 4
- freq_shift: float32 [4096], P('node'), may hold values from -4 to 4
- nbr_list: int32 [8, 6], P('node'), may hold values from -1 to 7, as said below
- send_nodes: int32 [8, 6, 32], P('node'), may hold values from 0 to 511, as said below
- adjacency: int32 [8, 4096], P(None, 'node'), may hold values from 0 to 703, as said below
Outputs:
- action_new: float32 [36, 36, 4096], P('freq', None, 'node')
The draws below stay inside these ranges and needn't reach their ends.
Inputs may be any that keep to these rules, and one draw needn't show every extreme that they name: `nbr_list`: slot entries of subdomain p are distinct subdomains (p + o) or (p - o) modulo the number of subdomains, 1 <= o <= 3, or -1 for an empty slot; p + 1 and p - 1 are always listed; if p lists q then q lists p. `send_nodes`: local node indices of the sending subdomain. `adjacency`: entries as in the first step; an entry at or above 512 never names an empty slot.
All inputs are finite; a program needn't handle non-finite values.
Results may differ from the reference program's by a relative error of at most 0.000088.
Values sent between devices are 32-bit elements; how exact they have to be, the bound alone decides.
A program may use at most 128 MiB of HBM per device.

```python
import math
import jax
import jax.numpy as jnp

FREQ = 36
DIR = 36
ND = 512
DEG = 8
REACH = 3
ITERS = 3
NB = 6
H = 32
NODES = 4096
N_NODE = 8


def neighbour_table(key):
    base = jax.random.fold_in(key, 11)
    subdomain = jnp.arange(N_NODE)
    columns = []
    for reach in range(1, REACH + 1):
        if reach == 1:
            linked = jnp.ones((N_NODE,), jnp.int32)
        else:
            linked = jax.random.randint(jax.random.fold_in(base, reach), (N_NODE,), 0, 2)
        upward = jnp.where(linked > 0, (subdomain + reach) % N_NODE, -1)
        downward = jnp.where(jnp.roll(linked, reach) > 0, (subdomain - reach) % N_NODE, -1)
        columns.append(upward)
        columns.append(downward)
    candidates = jnp.stack(columns, axis=1)
    scores = jax.random.randint(jax.random.fold_in(base, 99), (N_NODE, NB), 0, 1 << 16) * NB + jnp.arange(NB)[None, :]
    order = jnp.argsort(scores, axis=1)
    return jnp.take_along_axis(candidates, order, axis=1).astype(jnp.int32)


def draw_nbr_list(key, part):
    return neighbour_table(key)


def draw_send_nodes(key, part):
    return jax.random.randint(jax.random.fold_in(key, 5), (N_NODE, NB, H), 0, ND).astype(jnp.int32)


def draw_adjacency(key, part):
    table = neighbour_table(key)
    degree = jax.random.randint(jax.random.fold_in(key, 21), (N_NODE, ND), 3, DEG + 1)
    own_index = jnp.arange(ND)
    nearby = (own_index[None, None, :] + jax.random.randint(jax.random.fold_in(key, 22), (DEG, N_NODE, ND), 1, ND)) % ND
    halo_pos = jax.random.randint(jax.random.fold_in(key, 23), (DEG, N_NODE, ND), 0, NB * H)
    slot_live = jnp.repeat(table >= 0, H, axis=1)
    halo_live = jnp.take_along_axis(jnp.broadcast_to(slot_live[None], (DEG, N_NODE, NB * H)), halo_pos, axis=2)
    use_halo = (jax.random.randint(jax.random.fold_in(key, 24), (DEG, N_NODE, ND), 0, 100) < 15) & halo_live
    entry = jnp.where(use_halo, ND + halo_pos, nearby)
    scores = jax.random.randint(jax.random.fold_in(key, 25), (N_NODE, ND), 0, 1 << 16) * ND + own_index[None, :]
    ranking = jnp.argsort(jnp.argsort(scores, axis=1), axis=1)
    covered = ranking < NB * H
    cover_pos = jnp.where(covered, ranking, 0)
    cover_live = covered & jnp.take_along_axis(slot_live, cover_pos, axis=1)
    first = jnp.where(cover_live, ND + cover_pos, entry[0])
    entry = entry.at[0].set(first)
    levels = jnp.arange(DEG)[:, None, None]
    entry = jnp.where(levels < degree[None], entry, own_index[None, None, :])
    return entry.reshape(DEG, N_NODE * ND).astype(jnp.int32)


def steps_of(stream_key, shape, split, smallest, high):
    def one(dim, parts):
        draws = jax.random.uniform(jax.random.fold_in(jax.random.fold_in(stream_key, 6), dim), (parts,), jnp.float32, smallest / len(split), high / len(split))
        return jnp.repeat(jnp.exp(draws), shape[dim] // parts).reshape((-1,) + (1,) * (len(shape) - dim - 1))

    factor_of = one(*split[0])
    for cut in split[1:]:
        factor_of = factor_of * one(*cut)
    return factor_of


def scatter_about(own_key, extent, deviation, bound, cuts=(), held_as=jnp.bfloat16):
    result = deviation * jax.random.normal(own_key, extent, jnp.float32)
    if cuts:
        result = result * steps_of(own_key, extent, cuts, -0.22, 0.18)
    return jnp.clip(result, -bound, bound).astype(held_as)


def setup_inputs(seed: int = 0) -> dict:
    splits = jax.random.split(jax.random.key(seed), 11)
    action_old = jnp.clip(jnp.exp(math.log(2.0) - 3.6888794 * jax.random.uniform(splits[0], (FREQ, DIR, NODES), jnp.float32) ** steps_of(splits[0], (FREQ, DIR, NODES), ((0, 4), (2, 8)), -0.2, 0.2)), 0.05, 2.0)
    source = scatter_about(splits[1], (FREQ, DIR, NODES), 0.3, 4.0, ((0, 4), (2, 8)), jnp.float32)
    time_weight = jnp.clip(jnp.exp(math.log(4.0) - 2.0794415 * jax.random.uniform(splits[2], (NODES,), jnp.float32) ** steps_of(splits[2], (NODES,), ((0, 8),), -0.2, 0.2)), 0.5, 4.0)
    group_speed = jnp.clip(jnp.exp(math.log(3.0) - 2.3025851 * jax.random.uniform(splits[3], (FREQ,), jnp.float32) ** steps_of(splits[3], (FREQ,), ((0, 4),), -0.2, 0.2)), 0.3, 3.0)
    normals = scatter_about(splits[4], (2, DEG, NODES), 0.5, 3.0, ((2, 8),), jnp.float32)
    refract = scatter_about(splits[5], (NODES,), 0.6, 4.0, ((0, 8),), jnp.float32)
    freq_shift = scatter_about(splits[6], (NODES,), 0.6, 4.0, ((0, 8),), jnp.float32)
    nbr_list = draw_nbr_list(jax.random.fold_in(splits[10], 71), 0)
    send_nodes = draw_send_nodes(jax.random.fold_in(splits[10], 71), 0)
    adjacency = draw_adjacency(jax.random.fold_in(splits[10], 71), 0)
    return dict(action_old=action_old, source=source, time_weight=time_weight, group_speed=group_speed, normals=normals, refract=refract, freq_shift=freq_shift, nbr_list=nbr_list, send_nodes=send_nodes, adjacency=adjacency)


def reference(action_old, source, time_weight, group_speed, normals, refract, freq_shift, nbr_list, send_nodes, adjacency):
    count = nbr_list.shape[0]
    slots = nbr_list.shape[1]
    width = send_nodes.shape[2]
    local = action_old.shape[2] // count
    angles = 2.0 * math.pi * jnp.arange(DIR).astype(jnp.float32) / DIR
    cosine = jnp.cos(angles)
    sine = jnp.sin(angles)
    valid = nbr_list >= 0
    partner = jnp.where(valid, nbr_list, 0).astype(jnp.int32)
    backward = nbr_list[partner]
    subdomain = jnp.arange(count).astype(jnp.int32)
    slot_ids = jnp.arange(slots).astype(jnp.int32)
    reverse = jnp.sum(jnp.where(backward == subdomain[:, None, None], slot_ids[None, None, :], 0), axis=2).astype(jnp.int32)
    picked = send_nodes[partner, reverse]
    table = (partner[:, :, None] * local + picked).reshape(count, slots * width)
    entries = adjacency.reshape(DEG, count, local)
    position = jnp.clip(entries - local, 0, slots * width - 1)
    remote = jnp.take_along_axis(jnp.broadcast_to(table[None], (DEG, count, slots * width)), position, axis=2)
    global_index = jnp.where(entries < local, subdomain[None, :, None] * local + entries, remote)
    global_index = global_index.reshape(DEG, count * local).astype(jnp.int32)
    own_index = jnp.arange(local).astype(jnp.int32)
    used = (entries != own_index[None, None, :]).reshape(DEG, count * local)

    def flux(k):
        return group_speed[:, None, None] * (cosine[None, :, None] * normals[0, k][None, None, :] + sine[None, :, None] * normals[1, k][None, None, :])

    turning = refract[None, :] * cosine[:, None]
    diagonal = time_weight[None, None, :] + jnp.abs(turning)[None] + jnp.abs(freq_shift)[None, None, :]
    for k in range(DEG):
        diagonal = diagonal + jnp.where(used[k][None, None, :], jnp.maximum(flux(k), 0.0), 0.0)
    steady = time_weight[None, None, :] * action_old + source
    spectra = action_old
    zero_band = jnp.zeros_like(spectra[:1])
    for step in range(ITERS):
        inflow = jnp.maximum(turning, 0.0)[None] * jnp.roll(spectra, 1, axis=1) + jnp.maximum(-turning, 0.0)[None] * jnp.roll(spectra, -1, axis=1)
        lower = jnp.concatenate([zero_band, spectra[:-1]], axis=0)
        upper = jnp.concatenate([spectra[1:], zero_band], axis=0)
        inflow = inflow + jnp.maximum(freq_shift, 0.0)[None, None, :] * lower + jnp.maximum(-freq_shift, 0.0)[None, None, :] * upper
        for k in range(DEG):
            beside = jnp.take(spectra, global_index[k], axis=2)
            inflow = inflow + jnp.where(used[k][None, None, :], jnp.maximum(-flux(k), 0.0), 0.0) * beside
        spectra = (steady + inflow) / diagonal
    return spectra
```

```python
import functools
import math

import jax
import jax.numpy as jnp
import numpy as np
from jax import lax
from jax.experimental import pallas as pl
from jax.experimental.pallas import tpu as pltpu
from jax.sharding import PartitionSpec as P

REACH = 3
ITERS = 3
MESH = pl.DeviceIdType.MESH
OFFSETS = [sign * reach for reach in range(1, REACH + 1) for sign in (1, -1)]


def ceil_to(value, unit):
    return -(-value // unit) * unit


def split(value):
    high = value.astype(jnp.bfloat16)
    low = (value - high.astype(jnp.float32)).astype(jnp.bfloat16)
    return high, low


def dot(a, b):
    return jnp.dot(a, b, preferred_element_type=jnp.float32)


def kernel(
    count,
    fcount,
    speed,
    nbrs,
    picks,
    adjacency,
    time_weight,
    refract,
    freq_shift,
    normals,
    trig,
    action_old,
    source,
    out,
    spectra,
    steady,
    inverse,
    weights,
    turns,
    pieces,
    pick_matrix,
    selector,
    halo_selector,
    halo_pieces,
    gathered,
    staged,
    parcels,
    landed,
    bands_landed,
    send_sems,
    recv_sems,
):
    bands, angles, local = action_old.shape
    padded = turns.shape[1]
    slots, width = picks.shape[1], picks.shape[2]
    degree = adjacency.shape[0]
    rows = bands * padded
    wide = landed.shape[2]
    halo = slots * width
    halo_wide = halo_selector.shape[1]
    me = lax.axis_index("node")
    fme = lax.axis_index("freq")
    targets = [lax.rem(me + o + count, count) for o in OFFSETS]
    anchors = [lax.rem(me - o + count, count) for o in OFFSETS]
    above = lax.rem(fme + 1, fcount)
    below = lax.rem(fme + fcount - 1, fcount)
    partners = [{"node": t} for t in targets] + [{"freq": above}, {"freq": below}]

    barrier = pltpu.get_barrier_semaphore()
    for partner in partners:
        pl.semaphore_signal(barrier, inc=1, device_id=partner, device_id_type=MESH)

    def block(f):
        return pl.ds(f * padded, padded)

    def copies(step):
        result = []
        for j in range(len(OFFSETS)):
            piece = pl.ds(j * width, width)
            result.append((parcels.at[step, piece], landed.at[step, piece]))
        result.append((spectra.at[step, block(bands - 1)], bands_landed.at[step, 0]))
        result.append((spectra.at[step, block(0)], bands_landed.at[step, 1]))
        return [
            pltpu.make_async_remote_copy(
                src_ref=src,
                dst_ref=dst,
                send_sem=send_sems.at[step, i],
                recv_sem=recv_sems.at[step, i],
                device_id=partners[i],
                device_id_type=MESH,
            )
            for i, (src, dst) in enumerate(result)
        ]

    def prepare(step):
        high, low = split(spectra[step])
        pieces[0] = high
        pieces[1] = low
        staged[pl.ds(0, rows)] = dot(pieces[0], pick_matrix[...]) + dot(
            pieces[1], pick_matrix[...]
        )
        parcels[step] = jnp.transpose(staged[...])[:halo]

    def put(step, f, value):
        base = f * padded
        spectra[step, pl.ds(base, angles)] = value
        spectra[step, pl.ds(base + angles, 1)] = value[:1]
        spectra[step, pl.ds(base + padded - 1, 1)] = value[angles - 1 : angles]

    spectra[...] = jnp.zeros_like(spectra)
    if wide > rows:
        staged[pl.ds(rows, wide - rows)] = jnp.zeros((wide - rows, halo_wide), jnp.float32)
    for f in range(bands):
        put(0, f, action_old[f])
    chosen = []
    for target in targets:
        row = jnp.full((1, width), -1, jnp.int32)
        for s in range(slots):
            hit = jnp.full((1, width), nbrs[0, s], jnp.int32) == target
            row = jnp.where(hit, picks[0, pl.ds(s, 1)], row)
        chosen.append(row)
    if halo_wide > halo:
        chosen.append(jnp.full((1, halo_wide - halo), -1, jnp.int32))
    chosen = jnp.concatenate(chosen, axis=1)
    node_ids = lax.broadcasted_iota(jnp.int32, (local, halo_wide), 0)
    pick_matrix[...] = jnp.where(node_ids == chosen, 1.0, 0.0).astype(jnp.bfloat16)
    prepare(0)
    pl.semaphore_wait(barrier, len(partners))
    flights = [copies(0)]
    for copy in flights[0]:
        copy.start()

    repeats = local // trig.shape[2]
    cosine = jnp.concatenate([trig[0]] * repeats, axis=1)
    sine = jnp.concatenate([trig[1]] * repeats, axis=1)
    weight = time_weight[...].reshape(1, local)
    shift = freq_shift[...].reshape(1, local)
    turning = refract[...].reshape(1, local) * cosine
    turns[0] = jnp.maximum(turning, 0.0)
    turns[1] = jnp.maximum(-turning, 0.0)
    own = lax.broadcasted_iota(jnp.int32, (1, local), 1)
    outflow = jnp.zeros((padded, local), jnp.float32)
    for k in range(degree):
        entry = adjacency[pl.ds(k, 1)]
        used = jnp.where(entry != own, 1.0, 0.0)
        flow = (cosine * normals[0, pl.ds(k, 1)] + sine * normals[1, pl.ds(k, 1)]) * used
        outflow = outflow + jnp.maximum(flow, 0.0)
        weights[k] = jnp.maximum(-flow, 0.0)
        moved = entry
        for s in range(slots):
            place = jnp.zeros_like(entry)
            for j, anchor in enumerate(anchors):
                hit = jnp.full((1, local), nbrs[0, s], jnp.int32) == anchor
                place = jnp.where(hit, (j - s) * width, place)
            first = local + s * width
            inside = (entry >= first) & (entry < first + width)
            moved = moved + jnp.where(inside, place, 0)
        ids = lax.broadcasted_iota(jnp.int32, (local, local), 0)
        selector[k] = jnp.where(ids == moved, 1.0, 0.0).astype(jnp.bfloat16)
        halo_ids = lax.broadcasted_iota(jnp.int32, (halo_wide, local), 0) + local
        halo_selector[k] = jnp.where(halo_ids == moved, 1.0, 0.0).astype(jnp.bfloat16)
    still = weight + jnp.abs(turning) + jnp.abs(shift)
    for f in range(bands):
        inverse[block(f)] = 1.0 / (still + speed[f] * outflow)
        steady[block(f)] = jnp.zeros((padded, local), jnp.float32)
        steady[pl.ds(f * padded, angles)] = weight * action_old[f] + source[f]
    rising = jnp.maximum(shift, 0.0)
    falling = jnp.maximum(-shift, 0.0)
    has_below = jnp.where(jnp.full((1, local), fme, jnp.int32) > 0, rising, 0.0)
    has_above = jnp.where(jnp.full((1, local), fme, jnp.int32) < fcount - 1, falling, 0.0)

    for step in range(ITERS):
        gathered[...] = jnp.zeros_like(gathered)

        def near(k, carry):
            found = dot(pieces[0], selector[k]) + dot(pieces[1], selector[k])
            for f in range(bands):
                gathered[block(f)] += weights[k] * found[f * padded : (f + 1) * padded]
            return carry

        lax.fori_loop(0, degree, near, 0)
        for copy in flights[step]:
            copy.wait_recv()
        received = landed[step]
        if halo_wide > halo:
            received = jnp.concatenate(
                [received, jnp.zeros((halo_wide - halo, wide), jnp.float32)], axis=0
            )
        high, low = split(jnp.transpose(received)[:rows])
        halo_pieces[0] = high
        halo_pieces[1] = low

        def far(k, carry):
            found = dot(halo_pieces[0], halo_selector[k]) + dot(halo_pieces[1], halo_selector[k])
            for f in range(bands):
                gathered[block(f)] += weights[k] * found[f * padded : (f + 1) * padded]
            return carry

        lax.fori_loop(0, degree, far, 0)
        for f in range(bands):
            here = spectra[step, block(f)]
            total = steady[block(f)] + speed[f] * gathered[block(f)]
            total = total + turns[0] * pltpu.roll(here, 1, 0)
            total = total + turns[1] * pltpu.roll(here, padded - 1, 0)
            if f > 0:
                total = total + rising * spectra[step, block(f - 1)]
            else:
                total = total + has_below * bands_landed[step, 0]
            if f < bands - 1:
                total = total + falling * spectra[step, block(f + 1)]
            else:
                total = total + has_above * bands_landed[step, 1]
            value = (total * inverse[block(f)])[:angles]
            if step < ITERS - 1:
                put(step + 1, f, value)
            else:
                out[f] = value
        if step < ITERS - 1:
            prepare(step + 1)
            flights.append(copies(step + 1))
            for copy in flights[step + 1]:
                copy.start()
    for flight in flights:
        for copy in flight:
            copy.wait_send()


def body(count, fcount, *args):
    (
        action_old,
        source,
        time_weight,
        group_speed,
        normals,
        refract,
        freq_shift,
        nbr_list,
        send_nodes,
        adjacency,
    ) = args
    bands, angles, local = action_old.shape
    slots, width = send_nodes.shape[1:]
    degree = adjacency.shape[0]
    padded = ceil_to(angles + 2, 8)
    rows = bands * padded
    wide = ceil_to(rows, 128)
    halo = slots * width
    halo_wide = ceil_to(halo, 128)
    theta = 2.0 * math.pi * (np.arange(padded) % angles) / angles
    trig = np.stack([np.cos(theta), np.sin(theta)]).astype(np.float32)
    trig = jnp.asarray(np.ascontiguousarray(np.broadcast_to(trig[:, :, None], (2, padded, 128))))
    vmem = pl.BlockSpec(memory_space=pltpu.VMEM)
    smem = pl.BlockSpec(memory_space=pltpu.SMEM)
    f32, bf16 = jnp.float32, jnp.bfloat16
    copies = len(OFFSETS) + 2
    return pl.pallas_call(
        functools.partial(kernel, count, fcount),
        out_shape=jax.ShapeDtypeStruct(action_old.shape, f32),
        in_specs=[smem, smem] + [vmem] * 9,
        out_specs=vmem,
        scratch_shapes=[
            pltpu.VMEM((ITERS, rows, local), f32),
            pltpu.VMEM((rows, local), f32),
            pltpu.VMEM((rows, local), f32),
            pltpu.VMEM((degree, padded, local), f32),
            pltpu.VMEM((2, padded, local), f32),
            pltpu.VMEM((2, rows, local), bf16),
            pltpu.VMEM((local, halo_wide), bf16),
            pltpu.VMEM((degree, local, local), bf16),
            pltpu.VMEM((degree, halo_wide, local), bf16),
            pltpu.VMEM((2, rows, halo_wide), bf16),
            pltpu.VMEM((rows, local), f32),
            pltpu.VMEM((wide, halo_wide), f32),
            pltpu.VMEM((ITERS, halo, wide), f32),
            pltpu.VMEM((ITERS, halo, wide), f32),
            pltpu.VMEM((ITERS, 2, padded, local), f32),
            pltpu.SemaphoreType.DMA((ITERS, copies)),
            pltpu.SemaphoreType.DMA((ITERS, copies)),
        ],
        compiler_params=pltpu.CompilerParams(
            collective_id=0, has_side_effects=True, vmem_limit_bytes=48 * 1024 * 1024
        ),
    )(
        group_speed,
        nbr_list,
        send_nodes,
        adjacency,
        time_weight,
        refract,
        freq_shift,
        normals,
        trig,
        action_old,
        source,
    )


def solution(mesh):
    in_specs = (
        P("freq", None, "node"),
        P("freq", None, "node"),
        P("node"),
        P("freq"),
        P(None, None, "node"),
        P("node"),
        P("node"),
        P("node", None),
        P("node", None, None),
        P(None, "node"),
    )
    return jax.shard_map(
        functools.partial(body, mesh.shape["node"], mesh.shape["freq"]),
        mesh=mesh,
        in_specs=in_specs,
        out_specs=P("freq", None, "node"),
        check_vma=False,
    )
```

```python
import functools
import math

import jax
import jax.numpy as jnp
import numpy as np
from jax import lax
from jax.experimental import pallas as pl
from jax.experimental.pallas import tpu as pltpu
from jax.sharding import PartitionSpec as P

REACH = 3
ITERS = 3
CHUNKS = (2, 1)
UNROLL = 4
SEND_ORDER = (4, 5, 0, 1, 2, 3)
MESH = pl.DeviceIdType.MESH
OFFSETS = [sign * reach for reach in range(1, REACH + 1) for sign in (1, -1)]


def ceil_to(value, unit):
    return -(-value // unit) * unit


def split(value):
    high = value.astype(jnp.bfloat16)
    low = (value - high.astype(jnp.float32)).astype(jnp.bfloat16)
    return high, low


def dot(a, b):
    return jnp.dot(a, b, preferred_element_type=jnp.float32)


def kernel(
    count,
    fcount,
    speed_hbm,
    nbrs_hbm,
    picks_hbm,
    adjacency_hbm,
    time_weight_hbm,
    refract_hbm,
    freq_shift_hbm,
    normals_hbm,
    trig_hbm,
    action_hbm,
    source_hbm,
    out,
    speed,
    nbrs,
    picks,
    adjacency,
    time_weight,
    refract,
    freq_shift,
    normals,
    trig,
    action_old,
    source,
    load_sems,
    spectra,
    steady,
    inverse,
    weights,
    turns,
    pieces,
    pick_matrix,
    selector,
    halo_selector,
    halo_pieces,
    gathered,
    parcels,
    landed,
    bands_landed,
    send_sems,
    recv_sems,
):
    bands, angles, local = action_old.shape
    padded = turns.shape[1]
    slots, width = picks.shape[0], picks.shape[2]
    degree = adjacency.shape[0]
    rows = bands * padded
    wide = landed.shape[2]
    halo = slots * width
    halo_wide = halo_selector.shape[1]
    me = lax.axis_index("node")
    fme = lax.axis_index("freq")
    targets = [lax.rem(me + o + count, count) for o in OFFSETS]
    anchors = [lax.rem(me - o + count, count) for o in OFFSETS]
    above = lax.rem(fme + 1, fcount)
    below = lax.rem(fme + fcount - 1, fcount)
    partners = [{"node": t} for t in targets] + [{"freq": above}, {"freq": below}]

    barrier = pltpu.get_barrier_semaphore()
    for partner in partners:
        pl.semaphore_signal(barrier, inc=1, device_id=partner, device_id_type=MESH)

    names = [
        (action_hbm, action_old),
        (nbrs_hbm, nbrs),
        (picks_hbm, picks),
        (adjacency_hbm, adjacency),
        (normals_hbm, normals),
        (trig_hbm, trig),
        (refract_hbm, refract),
        (time_weight_hbm, time_weight),
        (freq_shift_hbm, freq_shift),
        (speed_hbm, speed),
        (source_hbm, source),
    ]
    loads = [pltpu.make_async_copy(a, b, load_sems.at[i]) for i, (a, b) in enumerate(names)]
    for load in loads:
        load.start()

    def neighbour(s, lanes):
        return jnp.broadcast_to(nbrs[:, s : s + 1], (1, lanes))

    def block(f):
        return pl.ds(f * padded, padded)

    group = 128 // padded
    used_rows = group * padded
    bounds = [sum(CHUNKS[:c]) for c in range(len(CHUNKS) + 1)]
    flights = {}

    def send(step, i, src, dst, partner):
        copy = pltpu.make_async_remote_copy(
            src_ref=src,
            dst_ref=dst,
            send_sem=send_sems.at[step, i],
            recv_sem=recv_sems.at[step, i],
            device_id=partners[partner],
            device_id_type=MESH,
        )
        copy.start()
        flights[step, i] = copy

    def send_chunk(step, c):
        lanes = pl.ds(bounds[c] * 128, CHUNKS[c] * 128)
        for j in SEND_ORDER:
            piece = (step, pl.ds(j * width, width), lanes)
            send(step, c * len(OFFSETS) + j, parcels.at[piece], landed.at[piece], j)

    def send_band(step, up):
        i = len(OFFSETS) * len(CHUNKS) + up
        src = spectra.at[step, block(bands - 1 if up else 0)]
        send(step, i, src, bands_landed.at[step, 1 - up], len(OFFSETS) + 1 - up)

    def prepare(step, c):
        rows_c = pl.ds(bounds[c] * used_rows, CHUNKS[c] * used_rows)
        high, low = split(spectra[step, rows_c])
        pieces[0, rows_c] = high
        pieces[1, rows_c] = low
        found = dot(high, pick_matrix[...]) + dot(low, pick_matrix[...])
        for g in range(CHUNKS[c]):
            part = found[g * used_rows : (g + 1) * used_rows]
            if used_rows < 128:
                fill = jnp.zeros((128 - used_rows, halo_wide), jnp.float32)
                part = jnp.concatenate([part, fill], axis=0)
            lanes = pl.ds((bounds[c] + g) * 128, 128)
            parcels[step, :, lanes] = jnp.transpose(part)[:halo]

    def put(step, f, value):
        base = f * padded
        spectra[step, pl.ds(base, angles)] = value
        spectra[step, pl.ds(base + angles, 1)] = value[:1]
        spectra[step, pl.ds(base + padded - 1, 1)] = value[angles - 1 : angles]

    spectra[...] = jnp.zeros_like(spectra)
    loads[0].wait()
    for f in range(bands):
        put(0, f, action_old[f])
    for load in loads[1:3]:
        load.wait()
    chosen = []
    for target in targets:
        row = jnp.full((1, width), -1, jnp.int32)
        for s in range(slots):
            hit = neighbour(s, width) == target
            row = jnp.where(hit, picks[s], row)
        chosen.append(row)
    if halo_wide > halo:
        chosen.append(jnp.full((1, halo_wide - halo), -1, jnp.int32))
    chosen = jnp.concatenate(chosen, axis=1)
    node_ids = lax.broadcasted_iota(jnp.int32, (local, halo_wide), 0)
    pick_matrix[...] = jnp.where(node_ids == chosen, 1.0, 0.0).astype(jnp.bfloat16)
    for c in range(len(CHUNKS)):
        prepare(0, c)
    for load in loads[3:]:
        load.wait()

    repeats = local // trig.shape[2]
    cosine = jnp.concatenate([trig[0]] * repeats, axis=1)
    sine = jnp.concatenate([trig[1]] * repeats, axis=1)
    weight = time_weight[...].reshape(1, local)
    shift = freq_shift[...].reshape(1, local)
    turning = refract[...].reshape(1, local) * cosine
    turns[0] = jnp.maximum(turning, 0.0)
    turns[1] = jnp.maximum(-turning, 0.0)
    own = lax.broadcasted_iota(jnp.int32, (1, local), 1)
    outflow = jnp.zeros((padded, local), jnp.float32)
    for k in range(degree):
        entry = adjacency[pl.ds(k, 1)]
        used = jnp.where(entry != own, 1.0, 0.0)
        flow = (cosine * normals[0, pl.ds(k, 1)] + sine * normals[1, pl.ds(k, 1)]) * used
        outflow = outflow + jnp.maximum(flow, 0.0)
        weights[k] = jnp.maximum(-flow, 0.0)
        moved = entry
        for s in range(slots):
            place = jnp.zeros_like(entry)
            for j, anchor in enumerate(anchors):
                hit = neighbour(s, local) == anchor
                place = jnp.where(hit, (j - s) * width, place)
            first = local + s * width
            inside = (entry >= first) & (entry < first + width)
            moved = moved + jnp.where(inside, place, 0)
        ids = lax.broadcasted_iota(jnp.int32, (local, local), 0)
        selector[k] = jnp.where(ids == moved, 1.0, 0.0).astype(jnp.bfloat16)
        halo_ids = lax.broadcasted_iota(jnp.int32, (halo_wide, local), 0) + local
        halo_selector[k] = jnp.where(halo_ids == moved, 1.0, 0.0).astype(jnp.bfloat16)
    still = weight + jnp.abs(turning) + jnp.abs(shift)
    speeds = speed[...].reshape(1, bands)
    gain = [jnp.broadcast_to(speeds[:, f : f + 1], (1, local)) for f in range(bands)]
    for f in range(bands):
        inverse[block(f)] = 1.0 / (still + gain[f] * outflow)
        steady[block(f)] = jnp.zeros((padded, local), jnp.float32)
        steady[pl.ds(f * padded, angles)] = weight * action_old[f] + source[f]
    rising = jnp.maximum(shift, 0.0)
    falling = jnp.maximum(-shift, 0.0)
    has_below = jnp.where(jnp.full((1, local), fme, jnp.int32) > 0, rising, 0.0)
    has_above = jnp.where(jnp.full((1, local), fme, jnp.int32) < fcount - 1, falling, 0.0)

    pl.semaphore_wait(barrier, len(partners))
    for c in range(len(CHUNKS)):
        send_chunk(0, c)
    send_band(0, 0)
    send_band(0, 1)

    for step in range(ITERS):
        gathered[...] = jnp.zeros_like(gathered)

        def near(i, carry):
            for u in range(UNROLL):
                k = i * UNROLL + u
                found = dot(pieces[0], selector[k]) + dot(pieces[1], selector[k])
                for f in range(bands):
                    gathered[block(f)] += weights[k] * found[f * padded : (f + 1) * padded]
            return carry

        lax.fori_loop(0, degree // UNROLL, near, 0)
        for c in range(len(CHUNKS)):
            for j in range(len(OFFSETS)):
                flights[step, c * len(OFFSETS) + j].wait_recv()
            base = bounds[c] * used_rows
            count_c = CHUNKS[c] * used_rows
            fs = range(bounds[c] * group, (bounds[c] + CHUNKS[c]) * group)
            for g in range(bounds[c], bounds[c + 1]):
                received = landed[step, :, pl.ds(g * 128, 128)]
                if halo_wide > halo:
                    fill = jnp.zeros((halo_wide - halo, 128), jnp.float32)
                    received = jnp.concatenate([received, fill], axis=0)
                high, low = split(jnp.transpose(received)[:used_rows])
                halo_pieces[0, pl.ds(g * used_rows, used_rows)] = high
                halo_pieces[1, pl.ds(g * used_rows, used_rows)] = low

            def far(i, carry):
                for u in range(UNROLL):
                    k = i * UNROLL + u
                    found = dot(halo_pieces[0, pl.ds(base, count_c)], halo_selector[k])
                    found += dot(halo_pieces[1, pl.ds(base, count_c)], halo_selector[k])
                    for n, f in enumerate(fs):
                        part = found[n * padded : (n + 1) * padded]
                        gathered[block(f)] += weights[k] * part
                return carry

            lax.fori_loop(0, degree // UNROLL, far, 0)
            if 0 in fs:
                flights[step, len(OFFSETS) * len(CHUNKS) + 1].wait_recv()
            if bands - 1 in fs:
                flights[step, len(OFFSETS) * len(CHUNKS)].wait_recv()
            for f in fs:
                here = spectra[step, block(f)]
                total = steady[block(f)] + gain[f] * gathered[block(f)]
                total = total + turns[0] * pltpu.roll(here, 1, 0)
                total = total + turns[1] * pltpu.roll(here, padded - 1, 0)
                if f > 0:
                    total = total + rising * spectra[step, block(f - 1)]
                else:
                    total = total + has_below * bands_landed[step, 0]
                if f < bands - 1:
                    total = total + falling * spectra[step, block(f + 1)]
                else:
                    total = total + has_above * bands_landed[step, 1]
                value = (total * inverse[block(f)])[:angles]
                if step < ITERS - 1:
                    put(step + 1, f, value)
                else:
                    out[f] = value
            if step < ITERS - 1:
                prepare(step + 1, c)
                send_chunk(step + 1, c)
                if 0 in fs:
                    send_band(step + 1, 0)
                if bands - 1 in fs:
                    send_band(step + 1, 1)
    for flight in flights.values():
        flight.wait_send()


def body(count, fcount, *args):
    (
        action_old,
        source,
        time_weight,
        group_speed,
        normals,
        refract,
        freq_shift,
        nbr_list,
        send_nodes,
        adjacency,
    ) = args
    bands, angles, local = action_old.shape
    slots, width = send_nodes.shape[1:]
    send_nodes = jnp.transpose(send_nodes, (1, 0, 2))
    degree = adjacency.shape[0]
    padded = ceil_to(angles + 2, 8)
    rows = bands * padded
    wide = sum(CHUNKS) * 128
    halo = slots * width
    halo_wide = ceil_to(halo, 128)
    theta = 2.0 * math.pi * (np.arange(padded) % angles) / angles
    trig = np.stack([np.cos(theta), np.sin(theta)]).astype(np.float32)
    trig = jnp.asarray(np.ascontiguousarray(np.broadcast_to(trig[:, :, None], (2, padded, 128))))
    vmem = pl.BlockSpec(memory_space=pltpu.VMEM)
    hbm = pl.BlockSpec(memory_space=pltpu.HBM)
    f32, bf16 = jnp.float32, jnp.bfloat16
    copies = len(OFFSETS) * len(CHUNKS) + 2
    assert (sum(CHUNKS) * (128 // padded), degree % UNROLL) == (bands, 0)
    operands = (
        group_speed,
        nbr_list,
        send_nodes,
        adjacency,
        time_weight,
        refract,
        freq_shift,
        normals,
        trig,
        action_old,
        source,
    )
    return pl.pallas_call(
        functools.partial(kernel, count, fcount),
        out_shape=jax.ShapeDtypeStruct(action_old.shape, f32),
        in_specs=[hbm] * len(operands),
        out_specs=vmem,
        scratch_shapes=[pltpu.VMEM(x.shape, x.dtype) for x in operands]
        + [
            pltpu.SemaphoreType.DMA((len(operands),)),
            pltpu.VMEM((ITERS, rows, local), f32),
            pltpu.VMEM((rows, local), f32),
            pltpu.VMEM((rows, local), f32),
            pltpu.VMEM((degree, padded, local), f32),
            pltpu.VMEM((2, padded, local), f32),
            pltpu.VMEM((2, rows, local), bf16),
            pltpu.VMEM((local, halo_wide), bf16),
            pltpu.VMEM((degree, local, local), bf16),
            pltpu.VMEM((degree, halo_wide, local), bf16),
            pltpu.VMEM((2, rows, halo_wide), bf16),
            pltpu.VMEM((rows, local), f32),
            pltpu.VMEM((ITERS, halo, wide), f32),
            pltpu.VMEM((ITERS, halo, wide), f32),
            pltpu.VMEM((ITERS, 2, padded, local), f32),
            pltpu.SemaphoreType.DMA((ITERS, copies)),
            pltpu.SemaphoreType.DMA((ITERS, copies)),
        ],
        compiler_params=pltpu.CompilerParams(
            collective_id=0, has_side_effects=True, vmem_limit_bytes=48 * 1024 * 1024
        ),
    )(*operands)


def solution(mesh):
    in_specs = (
        P("freq", None, "node"),
        P("freq", None, "node"),
        P("node"),
        P("freq"),
        P(None, None, "node"),
        P("node"),
        P("node"),
        P("node", None),
        P("node", None, None),
        P(None, "node"),
    )
    return jax.shard_map(
        functools.partial(body, mesh.shape["node"], mesh.shape["freq"]),
        mesh=mesh,
        in_specs=in_specs,
        out_specs=P("freq", None, "node"),
        check_vma=False,
    )
```
